256 devices in a mesh: chan: 16 (over z_hi, y, core), prof: 16 (over z_lo, x).
Axes of the slice: x: 4, y: 4, z: 8 (z_hi: 2, z_lo: 4; z = z_hi * 4 + z_lo), core: 2. Of those that a mesh axis runs over, the one named last changes fastest.
Arguments:
- observed: bfloat16 [256, 8448], P('prof', 'chan'), may hold values from -6 to 6
- eigvec: bfloat16 [8448, 300], P('chan'), may hold values from -0.0625 to 0.0625
- jacobian: bfloat16 [256, 8448, 400], P('prof', 'chan'), may hold values from -0.44921875 to 0.44921875
- radiance_base: bfloat16 [8448], P('chan'), may hold values from -1 to 1
- curvature: bfloat16 [8448], P('chan'), may hold values from -0.29882812 to 0.29882812
- block_mask: int32 [256, 256], P('prof', 'chan'), may hold values 0 or 1
- pc_weight: float32 [300], replicated, may hold values from 0.2 to 2
- prior_prec: float32 [400], replicated, may hold values from 0.3 to 3
- prior_mean: float32 [256, 400], P(('prof', 'chan')), may hold values from -6 to 6
- state0: float32 [256, 400], P(('prof', 'chan')), may hold values from -6 to 6
Outputs:
- states: float32 [256, 400], P(('prof', 'chan'))
The draws below stay inside these ranges and needn't reach their ends.
All inputs are finite; a program needn't handle non-finite values. No bound on the sum of `block_mask` on one device may be relied on, other than what follows from the above.
Results may differ from the reference program's by a relative error of at most 0.006.
Values may be sent and summed in bfloat16 or wider, within the bound.
No kernel may reach another device: no remote copies, remote signals or barrier semaphores. Data moves between devices by JAX's collectives and lax.ppermute only.
A program may use at most 128 MiB of HBM per device.

```python
import math
import jax
import jax.numpy as jnp
from jax import lax

C = 8448
K = 300
S = 400
NBLK = 256
ITERS = 2
PROFILES = 256


def place_ends(values, key, smallest, top_value):
    longest = values.shape.index(max(values.shape))
    spots = []
    for shift in (0, 1):
        where = [jax.random.randint(jax.random.fold_in(key, axis), (), 0, length) for axis, length in enumerate(values.shape)]
        where[longest] = (where[longest] + shift) % values.shape[longest]
        spots.append(tuple(where))
    return values.at[spots[0]].set(smallest).at[spots[1]].set(top_value)


def block_scale(stream_key, extent, cuts, least, largest):
    gain, own = 1.0, jax.random.fold_in(stream_key, 6)
    for axis_at, blocks in cuts:
        steps = jnp.exp(jax.random.uniform(jax.random.fold_in(own, axis_at), (blocks,), jnp.float32, least / len(cuts), largest / len(cuts)))
        gain = gain * jnp.repeat(steps, extent[axis_at] // blocks).reshape([-1 if axis == axis_at else 1 for axis in range(len(extent))])
    return gain


def normal_values(own_key, shape, width, limit, shards=(), kind=jnp.bfloat16):
    level = block_scale(own_key, shape, shards, -0.22, 0.18) if shards else 1.0
    array = jax.random.normal(own_key, shape, jnp.float32) * width * level
    return jnp.minimum(jnp.maximum(array, -limit), limit).astype(kind)


def setup_inputs(seed: int = 0) -> dict:
    arg_keys = jax.random.split(jax.random.key(seed), 11)
    observed = normal_values(arg_keys[0], (PROFILES, C), 1.0, 6.0, ((0, 16), (1, 16)))
    eigvec = normal_values(arg_keys[1], (C, K), C ** -0.5, 0.0625, ((0, 16),))
    jacobian = normal_values(arg_keys[2], (PROFILES, C, S), 0.15, 0.44921875, ((0, 16), (1, 16)))
    radiance_base = jnp.clip(jax.random.uniform(arg_keys[3], (C,), jnp.float32, -1.0, 1.0) * block_scale(arg_keys[3], (C,), ((0, 16),), -0.4, 0.0), -1.0, 1.0).astype(jnp.bfloat16)
    curvature = jnp.clip(jax.random.uniform(arg_keys[4], (C,), jnp.float32, -0.29882812, 0.29882812) * block_scale(arg_keys[4], (C,), ((0, 16),), -0.4, 0.0), -0.29882812, 0.29882812).astype(jnp.bfloat16)
    block_mask = place_ends((jax.random.randint(arg_keys[5], (PROFILES, NBLK), 0, 4) < 3).astype(jnp.int32), jax.random.fold_in(arg_keys[5], 1), 0, 1)
    pc_weight = jnp.clip(jnp.exp(jax.random.uniform(arg_keys[6], (K,), jnp.float32, math.log(0.2), math.log(2.0))), 0.2, 2.0)
    prior_prec = jnp.clip(jnp.exp(jax.random.uniform(arg_keys[7], (S,), jnp.float32, math.log(0.3), math.log(3.0))), 0.3, 3.0)
    prior_mean = normal_values(arg_keys[8], (PROFILES, S), 1.0, 6.0, ((0, 256),), jnp.float32)
    state0 = normal_values(arg_keys[9], (PROFILES, S), 1.0, 6.0, ((0, 256),), jnp.float32)
    return dict(observed=observed, eigvec=eigvec, jacobian=jacobian, radiance_base=radiance_base, curvature=curvature, block_mask=block_mask, pc_weight=pc_weight, prior_prec=prior_prec, prior_mean=prior_mean, state0=state0)


def solve_step(states, pc_resid, pc_jacob, pc_weight, prior_prec, prior_mean):
    highest = lax.Precision.HIGHEST
    weighted_jac = pc_jacob * pc_weight[None, :, None]
    normal = jnp.einsum('rks,rkt->rst', weighted_jac, pc_jacob, precision=highest)
    normal = normal + jnp.eye(pc_jacob.shape[2], dtype=jnp.float32)[None] * prior_prec[None, None, :]
    gradient = jnp.einsum('rks,rk->rs', pc_jacob, pc_weight[None, :] * pc_resid, precision=highest)
    gradient = gradient + prior_prec[None, :] * (states - prior_mean)
    factor = jnp.linalg.cholesky(normal)

    def one_solve(fac, vec):
        return jax.scipy.linalg.cho_solve((fac, True), vec)
    update = jax.vmap(one_solve)(factor, gradient)
    return states - update

def reference(observed, eigvec, jacobian, radiance_base, curvature, block_mask, pc_weight, prior_prec, prior_mean, state0):
    block_width = C // NBLK
    valid_mask = jnp.repeat(block_mask.astype(jnp.float32), block_width, axis=1)
    shift_f = radiance_base.astype(jnp.float32)
    curve_f = curvature.astype(jnp.float32)
    eig_f = eigvec.astype(jnp.float32)
    highest = lax.Precision.HIGHEST
    blocks = 16
    count = PROFILES // blocks

    def retrieve(pieces):
        states, spectra, valid, pmean, jac_bf = pieces
        jac_f = jac_bf.astype(jnp.float32)
        for iteration in range(ITERS):
            state_bf = states.astype(jnp.bfloat16)
            linear = jnp.einsum('rs,rcs->rc', state_bf.astype(jnp.float32), jac_f, precision=highest)
            misfit = (valid * (shift_f + linear + 0.5 * curve_f * linear * linear - spectra.astype(jnp.float32))).astype(jnp.bfloat16)
            slope = valid * (1.0 + curve_f * linear)
            weighted = (slope[:, :, None] * eig_f[None]).astype(jnp.bfloat16)
            pc_resid = jnp.dot(misfit.astype(jnp.float32), eigvec.astype(jnp.float32), preferred_element_type=jnp.float32)
            pc_jacob = jnp.einsum('rck,rcs->rks', weighted.astype(jnp.float32), jac_f, precision=highest)
            states = solve_step(states, pc_resid, pc_jacob, pc_weight, prior_prec, pmean)
        return states
    shaped = (state0.reshape(count, blocks, S), observed.reshape(count, blocks, C), valid_mask.reshape(count, blocks, C), prior_mean.reshape(count, blocks, S), jacobian.reshape(count, blocks, C, S))
    result = lax.map(retrieve, shaped)
    return result.reshape(PROFILES, S)
```

```python
import functools

import jax
import jax.numpy as jnp
from jax import lax
from jax.experimental import pallas as pl
from jax.experimental.pallas import tpu as pltpu
from jax.sharding import PartitionSpec as P

ITERS = 2
HIGHEST = lax.Precision.HIGHEST
f32, bf16 = jnp.float32, jnp.bfloat16

ROWS = 304
TOP = 128
LOW = ROWS - TOP
CUT = 3 * TOP + 16
FOLD = CUT + 3 * LOW
BLOCK = FOLD + 32
GRANT = pltpu.CompilerParams(vmem_limit_bytes=14 * 2**20)


def dot_nn(a, b, precision=HIGHEST):
    dims = (((1,), (0,)), ((), ()))
    return lax.dot_general(a, b, dims, precision=precision, preferred_element_type=f32)


def dot_nt(a, b, precision=HIGHEST):
    dims = (((1,), (1,)), ((), ()))
    return lax.dot_general(a, b, dims, precision=precision, preferred_element_type=f32)


def owner_of(dy, dz, dc):
    me = lax.axis_index("chan")
    z, y, core = lax.div(me, 8), lax.rem(lax.div(me, 2), 4), lax.rem(me, 2)
    return lax.rem(z + dz, 2) * 8 + lax.rem(y + dy, 4) * 2 + lax.rem(core + dc, 2)


def mask_kernel(mask_ref, valid_ref):
    blocks, width = mask_ref.shape[1], valid_ref.shape[1]
    owner = lax.broadcasted_iota(jnp.int32, (blocks, width), 0) * (width // blocks)
    channel = lax.broadcasted_iota(jnp.int32, (blocks, width), 1)
    spread = jnp.where((channel >= owner) & (channel < owner + width // blocks), 1.0, 0.0)
    valid_ref[...] = dot_nn(mask_ref[...].astype(f32).astype(bf16), spread.astype(bf16), None)


def valid_channels(block_mask, width):
    return pl.pallas_call(
        mask_kernel,
        out_shape=jax.ShapeDtypeStruct((block_mask.shape[0], width), f32),
        cost_estimate=pl.CostEstimate(flops=2 * 10**10, bytes_accessed=0, transcendentals=0),
        compiler_params=GRANT,
        name="valid_channels",
    )(block_mask)


def slope_kernel(*refs):
    fours, refs = refs[:4], refs[4:]
    observed_ref, valid_ref, base_ref, curve_ref, eig_ref, jac_ref = refs[:6]
    slope_ref, resid_ref, linear_ref = refs[6:]
    profiles, width = observed_ref.shape
    valid = valid_ref[...]
    state = jnp.concatenate([ref[...].astype(f32) for ref in fours], axis=0).astype(bf16)
    for slot in range(profiles):
        p = owner_of(slot // 4, slot // 2 % 2, slot % 2)
        linear_ref[pl.ds(p, 1), :] = dot_nn(state, jac_ref[p], None)[slot : slot + 1]
    linear = linear_ref[...]
    base = base_ref[...].astype(f32).reshape(1, width)
    curve = curve_ref[...].astype(f32).reshape(1, width)
    misfit = valid * (
        base + linear + 0.5 * curve * linear * linear - observed_ref[...].astype(f32)
    )
    slope_ref[...] = valid * (1.0 + curve * linear)
    resid = dot_nt(misfit.astype(bf16), eig_ref[...], None)
    resid_ref[...] = jnp.pad(resid, ((0, 0), (0, 384 - resid.shape[1])))


def slopes(fours, observed, valid, base, curve, eig_t, jac_t):
    profiles, states, width = jac_t.shape
    vmem = pl.BlockSpec(memory_space=pltpu.VMEM)
    return pl.pallas_call(
        slope_kernel,
        out_shape=(
            jax.ShapeDtypeStruct((profiles, width), f32),
            jax.ShapeDtypeStruct((profiles, 384), f32),
        ),
        in_specs=[vmem] * 10,
        out_specs=(vmem, vmem),
        scratch_shapes=[pltpu.VMEM((profiles, width), f32)],
        cost_estimate=pl.CostEstimate(flops=10**9, bytes_accessed=0, transcendentals=0),
        compiler_params=GRANT,
        name="slopes",
    )(*fours, observed, valid, base, curve, eig_t, jac_t)


def project_kernel(dy, slope_ref, resid_ref, eig_ref, jac_ref, keep_ref, send_ref):
    states = jac_ref.shape[1]

    def folded(part, group):
        part = jnp.pad(part, ((0, 8 * group - part.shape[0]), (0, 512 - states)))
        total = part[0:group]
        for i in range(1, 8):
            total += pltpu.roll(part[group * i : group * i + group], 16 * i, 1)
        return total

    def one(dz, dc, out_ref):
        p = owner_of(dy, dz, dc)
        weighted = (slope_ref[pl.ds(p, 1), :] * eig_ref[...].astype(f32)).astype(bf16)
        pc = dot_nt(weighted, jac_ref[p], None)
        pc = jnp.pad(pc, ((0, ROWS - pc.shape[0]), (0, 0)))
        for i in range(3):
            tile = pc[:, i * 128 : (i + 1) * 128]
            out_ref[dz, i * TOP : (i + 1) * TOP, :] = tile[:TOP]
            out_ref[dz, CUT + i * LOW : CUT + (i + 1) * LOW, :] = tile[TOP:]
        out_ref[dz, 3 * TOP : CUT, :] = folded(pc[:TOP, 384:states], 16)
        out_ref[dz, FOLD : FOLD + 24, :] = folded(pc[TOP:, 384:states], 24)
        resid = resid_ref[pl.ds(p, 1), :]
        high = resid.astype(bf16).astype(f32)
        low = resid - high
        rows = [part[:, 128 * i : 128 * i + 128] for part in (high, low) for i in range(3)]
        rows.append(jnp.zeros((2, 128), f32))
        out_ref[dz, FOLD + 24 : BLOCK, :] = jnp.concatenate(rows, axis=0)

    def step(dz, carry):
        one(dz, 1, send_ref)
        one(dz, 0, keep_ref)
        return carry

    lax.fori_loop(0, 2, step, 0)


def project(dy, slope, resid, eig_t, jac_t):
    vmem = pl.BlockSpec(memory_space=pltpu.VMEM)
    shape = (2, BLOCK, 128)
    return pl.pallas_call(
        functools.partial(project_kernel, dy),
        out_shape=(jax.ShapeDtypeStruct(shape, f32),) * 2,
        in_specs=[vmem] * 4,
        out_specs=(vmem, vmem),
        cost_estimate=pl.CostEstimate(flops=10**9, bytes_accessed=0, transcendentals=0),
        compiler_params=GRANT,
        name="project",
    )(slope, resid, eig_t, jac_t)


def spread_lane(tile, j):
    return jnp.broadcast_to(tile[:, j : j + 1], (8, 128))


def spread_row(tile, j):
    return jnp.broadcast_to(tile[j : j + 1, :], (8, 128))


def spd_inverse(tiles):
    sub = lax.broadcasted_iota(jnp.int32, (8, 128), 0)
    lane = lax.broadcasted_iota(jnp.int32, (8, 128), 1)
    count = len(tiles)
    units = [jnp.where(lane - 8 * i == sub, 1.0, 0.0) for i in range(count)]
    reduced = []
    cols = [spread_lane(tiles[0], j) for j in range(8)]
    for k in range(count):
        pivot, unit = tiles[k], units[k]
        follow = k + 1 < count
        ahead, coming, factors = [], [], []
        if follow:
            ahead = [spread_lane(tiles[k], 8 * k + 8 + j) for j in range(8)]
            coming = [spread_lane(tiles[k + 1], 8 * k + 8 + j) for j in range(8)]
            factors = [spread_lane(tiles[k + 1], 8 * k + j) for j in range(8)]
        diagonal = spread_row(cols[0], 0)
        scale = None
        for j in range(8):
            inverse = 1.0 / diagonal
            if j < 7:
                cross = cols[j] * spread_row(cols[j + 1], j)
                diagonal = spread_row(cols[j + 1], j + 1) - spread_row(cross, j + 1) * inverse
            scale = jnp.where(sub == j, inverse, scale) if j else inverse
            gain = jnp.where(sub == j, 0.0, cols[j] * inverse)

            def eliminated(value):
                return value - gain * spread_row(value, j)

            for m in range(j + 1, 8):
                cols[m] = eliminated(cols[m])
            pivot, unit = eliminated(pivot), eliminated(unit)
            ahead = [eliminated(value) for value in ahead]
        unit *= scale
        reduced.append(unit)
        if not follow:
            break
        pivot *= scale
        rows = [spread_row(pivot, j) for j in range(8)]
        unit_rows = [spread_row(unit, j) for j in range(8)]
        for i in range(k + 1, count):
            each = factors if i == k + 1 else [spread_lane(tiles[i], 8 * k + j) for j in range(8)]
            for j in range(8):
                tiles[i] = tiles[i] - each[j] * rows[j]
                units[i] = units[i] - each[j] * unit_rows[j]
        cols = []
        for value, start in zip(ahead, coming):
            value *= scale
            for m in range(8):
                start -= factors[m] * spread_row(value, m)
            cols.append(start)
    lower, scaled = jnp.concatenate(units, axis=0), jnp.concatenate(reduced, axis=0)
    dims = (((0,), (0,)), ((), ()))
    return lax.dot_general(lower, scaled, dims, precision=HIGHEST, preferred_element_type=f32)


def unfolded(block, rows, group):
    packed = block[3 * rows : 3 * rows + group]
    lane = lax.broadcasted_iota(jnp.int32, (group, 128), 1)
    last = [packed if i == 0 else pltpu.roll(packed, 128 - 16 * i, 1) for i in range(8)]
    last = jnp.concatenate([jnp.where(lane < 16, part, 0.0) for part in last], axis=0)
    tiles = [block[i * rows : (i + 1) * rows] for i in range(3)]
    return jnp.concatenate(tiles + [last[:rows]], axis=1)


def plus_diagonal(square, row):
    i0 = lax.broadcasted_iota(jnp.int32, square.shape, 0)
    i1 = lax.broadcasted_iota(jnp.int32, square.shape, 1)
    return square + jnp.where(i0 == i1, row, 0.0)


def tiles_of(square):
    return [square[i : i + 8] for i in range(0, square.shape[0], 8)]


def wide(row, size, fill=0.0):
    return jnp.pad(row, ((0, 0), (0, size - row.shape[1])), constant_values=fill)


def top_kernel(keep_ref, got_ref, prec_ref, weight_ref, jac_ref, inv_ref):
    block = keep_ref[...] + got_ref[...].astype(f32)
    jac = unfolded(block, TOP, 16) * wide(1.0 / jnp.sqrt(prec_ref[...]), 512)
    jac_ref[...] = jac
    s = plus_diagonal(dot_nt(jac, jac), 1.0 / weight_ref[...].reshape(1, -1)[:, :TOP])
    inv_ref[...] = spd_inverse(tiles_of(s))


def top_step(keep, got, prec, weight):
    return pl.pallas_call(
        top_kernel,
        out_shape=(
            jax.ShapeDtypeStruct((TOP, 512), f32),
            jax.ShapeDtypeStruct((TOP, TOP), f32),
        ),
        cost_estimate=pl.CostEstimate(flops=10**9, bytes_accessed=0, transcendentals=0),
        compiler_params=GRANT,
        name="top_step",
    )(keep, got, prec, weight)


def low_kernel(
    keep_ref, got_ref, top_ref, inv_ref, state_ref, prec_ref, mean_ref, weight_ref,
    out_ref, short_ref,
):
    block = keep_ref[...] + got_ref[...].astype(f32)
    root = jnp.sqrt(prec_ref[...])
    scale = wide(1.0 / root, 512)
    noise = wide(1.0 / weight_ref[...].reshape(1, -1)[:, TOP:], LOW, 1.0)
    low = unfolded(block, LOW, 24) * scale
    top, inv0 = top_ref[...], inv_ref[...]
    first = BLOCK - CUT - 8
    v = [block[first + i : first + i + 1] + block[first + 3 + i : first + 4 + i] for i in range(3)]
    v0 = jnp.broadcast_to(v[0], (8, 128))
    v12 = jnp.broadcast_to(jnp.concatenate(v[1:], axis=1)[:, :LOW], (8, LOW))
    shift = wide(root * (state_ref[...] - mean_ref[...]), 512)
    shift = jnp.broadcast_to(shift, (8, 512))
    v0 -= dot_nt(shift, top)
    v12 -= dot_nt(shift, low)
    s10 = dot_nt(low, top)
    t10 = dot_nn(s10, inv0)
    s = plus_diagonal(dot_nt(low, low), noise) - dot_nt(t10, s10)
    v12 -= dot_nt(v0, t10)
    inv1 = spd_inverse(tiles_of(s[:128, :128]))
    s21 = s[128:, :128]
    t21 = dot_nn(s21, inv1)
    s22 = s[128:, 128:] - dot_nt(t21, s21)
    s22 = jnp.pad(s22, ((0, 0), (0, 256 - LOW)))
    v1 = v12[:, :128]
    v2 = v12[:, 128:] - dot_nt(v1, t21)
    inv2 = spd_inverse(tiles_of(s22))[: LOW - 128]
    y2 = dot_nn(v2, inv2)[:, : LOW - 128]
    y1 = dot_nn(v1 - dot_nn(y2, s21), inv1)
    y12 = jnp.concatenate([y1, y2], axis=1)
    y0 = dot_nn(v0 - dot_nn(y12, s10), inv0)
    step = (dot_nn(y0, top) + dot_nn(y12, low)) * scale
    new = mean_ref[...] - step[0:1, : mean_ref.shape[1]]
    out_ref[...] = new
    short_ref[...] = new.astype(bf16)


def low_step(keep, got, top, inv0, state, prec, mean, weight):
    return pl.pallas_call(
        low_kernel,
        out_shape=(
            jax.ShapeDtypeStruct(mean.shape, f32),
            jax.ShapeDtypeStruct(mean.shape, bf16),
        ),
        cost_estimate=pl.CostEstimate(flops=10**9, bytes_accessed=0, transcendentals=0),
        compiler_params=GRANT,
        name="low_step",
    )(keep, got, top, inv0, state, prec, mean, weight)


def index_of(z, y, core):
    return z * 8 + y * 2 + core


MEMBERS = [(z, y, core) for z in range(2) for y in range(4) for core in range(2)]


def swap_core(value):
    return lax.ppermute(
        value, "chan", [(index_of(z, y, c), index_of(z, y, 1 - c)) for z, y, c in MEMBERS]
    )


def move_y(value, step):
    return lax.ppermute(
        value, "chan", [(index_of(z, y, c), index_of(z, (y + step) % 4, c)) for z, y, c in MEMBERS]
    )


def swap_z(value):
    return lax.ppermute(
        value, "chan", [(index_of(z, y, c), index_of(1 - z, y, c)) for z, y, c in MEMBERS]
    )


def gathered(value):
    pair = jnp.concatenate([value, swap_core(value)], axis=0)
    four = jnp.concatenate([pair, swap_z(pair)], axis=0)
    return [four] + [move_y(four, -dy) for dy in (1, 2, 3)]


def after(value, *others):
    return lax.optimization_barrier((value, *others))[0]


def local(
    observed, eigvec, jacobian, radiance_base, curvature, block_mask,
    pc_weight, prior_prec, prior_mean, state0,
):
    eig_t = eigvec.T
    jac_t = jnp.swapaxes(jacobian, 1, 2)
    prec = prior_prec.reshape(1, -1)

    def iterate(_, carry):
        state, short = carry
        fours = gathered(short)
        valid = valid_channels(after(block_mask, short), observed.shape[1])
        slope, resid = slopes(
            fours, observed, valid, radiance_base, curvature, eig_t, jac_t
        )

        def chip_sum(dy, here):
            keep, send = project(dy, here, resid, eig_t, jac_t)
            return keep, swap_core(send)

        def chunk(pair, part, dz):
            return pair[0][dz, part] + pair[1][dz, part]

        everything = slice(0, BLOCK)
        far = chip_sum(2, slope)
        ahead = chip_sum(1, slope)
        relay = [chunk(far, everything, dz).astype(bf16) for dz in range(2)]
        forth, back = move_y(relay[0], 1), move_y(relay[1], -1)
        later = after(slope, *relay)
        behind = chip_sum(3, later)
        own = chip_sum(0, after(later, behind[0]))
        both = []
        for part in (slice(0, CUT), slice(CUT, BLOCK)):
            up = [chunk(ahead, part, 0) + forth[part].astype(f32), chunk(ahead, part, 1)]
            down = [chunk(behind, part, 0), chunk(behind, part, 1) + back[part].astype(f32)]
            up = move_y(jnp.stack(up).astype(bf16), 1)
            down = move_y(jnp.stack(down).astype(bf16), -1)
            near = [
                chunk(own, part, dz) + up[dz].astype(f32) + down[dz].astype(f32)
                for dz in range(2)
            ]
            both.append((near[0], swap_z(near[1].astype(bf16))))
        top, inv0 = top_step(*both[0], prec, pc_weight)
        return low_step(*both[1], top, inv0, state, prec, prior_mean, pc_weight)

    return lax.fori_loop(0, ITERS, iterate, (state0, state0.astype(bf16)))[0]


def solution(mesh):
    return jax.shard_map(
        local,
        mesh=mesh,
        in_specs=(
            P("prof", "chan"),
            P("chan", None),
            P("prof", "chan", None),
            P("chan"),
            P("chan"),
            P("prof", "chan"),
            P(),
            P(),
            P(("prof", "chan"), None),
            P(("prof", "chan"), None),
        ),
        out_specs=P(("prof", "chan"), None),
        check_vma=False,
    )
```

```python
import functools

import jax
import jax.numpy as jnp
from jax import lax
from jax.experimental import pallas as pl
from jax.experimental.pallas import tpu as pltpu
from jax.sharding import PartitionSpec as P

ITERS = 2
HIGHEST = lax.Precision.HIGHEST
f32, bf16 = jnp.float32, jnp.bfloat16

ROWS = 304
TOP = 128
LOW = ROWS - TOP
CUT = 3 * TOP + 16
FOLD = CUT + 3 * LOW
BLOCK = FOLD + 32
GRANT = pltpu.CompilerParams(vmem_limit_bytes=14 * 2**20)


def dot_nn(a, b, precision=HIGHEST):
    dims = (((1,), (0,)), ((), ()))
    return lax.dot_general(a, b, dims, precision=precision, preferred_element_type=f32)


def dot_nt(a, b, precision=HIGHEST):
    dims = (((1,), (1,)), ((), ()))
    return lax.dot_general(a, b, dims, precision=precision, preferred_element_type=f32)


def owner_of(dy, dz, dc):
    me = lax.axis_index("chan")
    z, y, core = lax.div(me, 8), lax.rem(lax.div(me, 2), 4), lax.rem(me, 2)
    return lax.rem(z + dz, 2) * 8 + lax.rem(y + dy, 4) * 2 + lax.rem(core + dc, 2)


def mask_kernel(mask_ref, valid_ref):
    blocks, width = mask_ref.shape[1], valid_ref.shape[1]
    owner = lax.broadcasted_iota(jnp.int32, (blocks, width), 0) * (width // blocks)
    channel = lax.broadcasted_iota(jnp.int32, (blocks, width), 1)
    spread = jnp.where((channel >= owner) & (channel < owner + width // blocks), 1.0, 0.0)
    valid_ref[...] = dot_nn(mask_ref[...].astype(f32).astype(bf16), spread.astype(bf16), None)


def valid_channels(block_mask, width):
    return pl.pallas_call(
        mask_kernel,
        out_shape=jax.ShapeDtypeStruct((block_mask.shape[0], width), f32),
        cost_estimate=pl.CostEstimate(flops=2 * 10**10, bytes_accessed=0, transcendentals=0),
        compiler_params=GRANT,
        name="valid_channels",
    )(block_mask)


def slope_kernel(*refs):
    fours, refs = refs[:4], refs[4:]
    observed_ref, valid_ref, base_ref, curve_ref, eig_ref, jac_ref = refs[:6]
    slope_ref, resid_ref, linear_ref = refs[6:]
    profiles, width = observed_ref.shape
    valid = valid_ref[...]
    state = jnp.concatenate([ref[...].astype(f32) for ref in fours], axis=0).astype(bf16)
    for slot in range(profiles):
        p = owner_of(slot // 4, slot // 2 % 2, slot % 2)
        linear_ref[pl.ds(p, 1), :] = dot_nn(state, jac_ref[p], None)[slot : slot + 1]
    linear = linear_ref[...]
    base = base_ref[...].astype(f32).reshape(1, width)
    curve = curve_ref[...].astype(f32).reshape(1, width)
    misfit = valid * (
        base + linear + 0.5 * curve * linear * linear - observed_ref[...].astype(f32)
    )
    slope_ref[...] = valid * (1.0 + curve * linear)
    resid = dot_nt(misfit.astype(bf16), eig_ref[...], None)
    resid_ref[...] = jnp.pad(resid, ((0, 0), (0, 384 - resid.shape[1])))


def slopes(fours, observed, valid, base, curve, eig_t, jac_t):
    profiles, states, width = jac_t.shape
    vmem = pl.BlockSpec(memory_space=pltpu.VMEM)
    return pl.pallas_call(
        slope_kernel,
        out_shape=(
            jax.ShapeDtypeStruct((profiles, width), f32),
            jax.ShapeDtypeStruct((profiles, 384), f32),
        ),
        in_specs=[vmem] * 10,
        out_specs=(vmem, vmem),
        scratch_shapes=[pltpu.VMEM((profiles, width), f32)],
        cost_estimate=pl.CostEstimate(flops=10**9, bytes_accessed=0, transcendentals=0),
        compiler_params=GRANT,
        name="slopes",
    )(*fours, observed, valid, base, curve, eig_t, jac_t)


def project_kernel(dy, slope_ref, resid_ref, eig_ref, jac_ref, keep_ref, send_ref):
    states = jac_ref.shape[1]

    def folded(part, group):
        part = jnp.pad(part, ((0, 8 * group - part.shape[0]), (0, 512 - states)))
        total = part[0:group]
        for i in range(1, 8):
            total += pltpu.roll(part[group * i : group * i + group], 16 * i, 1)
        return total

    def one(dz, dc, out_ref):
        p = owner_of(dy, dz, dc)
        weighted = (slope_ref[pl.ds(p, 1), :] * eig_ref[...].astype(f32)).astype(bf16)
        pc = dot_nt(weighted, jac_ref[p], None)
        pc = jnp.pad(pc, ((0, ROWS - pc.shape[0]), (0, 0)))
        for i in range(3):
            tile = pc[:, i * 128 : (i + 1) * 128]
            out_ref[dz, i * TOP : (i + 1) * TOP, :] = tile[:TOP]
            out_ref[dz, CUT + i * LOW : CUT + (i + 1) * LOW, :] = tile[TOP:]
        out_ref[dz, 3 * TOP : CUT, :] = folded(pc[:TOP, 384:states], 16)
        out_ref[dz, FOLD : FOLD + 24, :] = folded(pc[TOP:, 384:states], 24)
        resid = resid_ref[pl.ds(p, 1), :]
        high = resid.astype(bf16).astype(f32)
        low = resid - high
        rows = [part[:, 128 * i : 128 * i + 128] for part in (high, low) for i in range(3)]
        rows.append(jnp.zeros((2, 128), f32))
        out_ref[dz, FOLD + 24 : BLOCK, :] = jnp.concatenate(rows, axis=0)

    def step(dz, carry):
        one(dz, 1, send_ref)
        one(dz, 0, keep_ref)
        return carry

    lax.fori_loop(0, 2, step, 0)


def project(dy, slope, resid, eig_t, jac_t):
    vmem = pl.BlockSpec(memory_space=pltpu.VMEM)
    shape = (2, BLOCK, 128)
    return pl.pallas_call(
        functools.partial(project_kernel, dy),
        out_shape=(jax.ShapeDtypeStruct(shape, f32),) * 2,
        in_specs=[vmem] * 4,
        out_specs=(vmem, vmem),
        cost_estimate=pl.CostEstimate(flops=10**9, bytes_accessed=0, transcendentals=0),
        compiler_params=GRANT,
        name="project",
    )(slope, resid, eig_t, jac_t)


def spread_lane(tile, j):
    return jnp.broadcast_to(tile[:, j : j + 1], (8, 128))


def spread_row(tile, j):
    return jnp.broadcast_to(tile[j : j + 1, :], (8, 128))


def spd_inverse(tiles):
    sub = lax.broadcasted_iota(jnp.int32, (8, 128), 0)
    lane = lax.broadcasted_iota(jnp.int32, (8, 128), 1)
    count = len(tiles)
    units = [jnp.where(lane - 8 * i == sub, 1.0, 0.0) for i in range(count)]
    reduced = []
    cols = [spread_lane(tiles[0], j) for j in range(8)]
    for k in range(count):
        pivot, unit = tiles[k], units[k]
        follow = k + 1 < count
        ahead, coming, factors = [], [], []
        if follow:
            ahead = [spread_lane(tiles[k], 8 * k + 8 + j) for j in range(8)]
            coming = [spread_lane(tiles[k + 1], 8 * k + 8 + j) for j in range(8)]
            factors = [spread_lane(tiles[k + 1], 8 * k + j) for j in range(8)]
        diagonal = spread_row(cols[0], 0)
        scale = None
        for j in range(8):
            inverse = 1.0 / diagonal
            if j < 7:
                cross = cols[j] * spread_row(cols[j + 1], j)
                diagonal = spread_row(cols[j + 1], j + 1) - spread_row(cross, j + 1) * inverse
            scale = jnp.where(sub == j, inverse, scale) if j else inverse
            gain = jnp.where(sub == j, 0.0, cols[j] * inverse)

            def eliminated(value):
                return value - gain * spread_row(value, j)

            for m in range(j + 1, 8):
                cols[m] = eliminated(cols[m])
            pivot, unit = eliminated(pivot), eliminated(unit)
            ahead = [eliminated(value) for value in ahead]
        unit *= scale
        reduced.append(unit)
        if not follow:
            break
        pivot *= scale
        rows = [spread_row(pivot, j) for j in range(8)]
        unit_rows = [spread_row(unit, j) for j in range(8)]
        for i in range(k + 1, count):
            each = factors if i == k + 1 else [spread_lane(tiles[i], 8 * k + j) for j in range(8)]
            for j in range(8):
                tiles[i] = tiles[i] - each[j] * rows[j]
                units[i] = units[i] - each[j] * unit_rows[j]
        cols = []
        for value, start in zip(ahead, coming):
            value *= scale
            for m in range(8):
                start -= factors[m] * spread_row(value, m)
            cols.append(start)
    lower, scaled = jnp.concatenate(units, axis=0), jnp.concatenate(reduced, axis=0)
    dims = (((0,), (0,)), ((), ()))
    return lax.dot_general(lower, scaled, dims, precision=HIGHEST, preferred_element_type=f32)


def unfolded(block, rows, group):
    packed = block[3 * rows : 3 * rows + group]
    lane = lax.broadcasted_iota(jnp.int32, (group, 128), 1)
    last = [packed if i == 0 else pltpu.roll(packed, 128 - 16 * i, 1) for i in range(8)]
    last = jnp.concatenate([jnp.where(lane < 16, part, 0.0) for part in last], axis=0)
    tiles = [block[i * rows : (i + 1) * rows] for i in range(3)]
    return jnp.concatenate(tiles + [last[:rows]], axis=1)


def plus_diagonal(square, row):
    i0 = lax.broadcasted_iota(jnp.int32, square.shape, 0)
    i1 = lax.broadcasted_iota(jnp.int32, square.shape, 1)
    return square + jnp.where(i0 == i1, row, 0.0)


def tiles_of(square):
    return [square[i : i + 8] for i in range(0, square.shape[0], 8)]


def wide(row, size, fill=0.0):
    return jnp.pad(row, ((0, 0), (0, size - row.shape[1])), constant_values=fill)


def top_kernel(keep_ref, got_ref, prec_ref, weight_ref, jac_ref, inv_ref):
    block = keep_ref[...] + got_ref[...].astype(f32)
    jac = unfolded(block, TOP, 16) * wide(1.0 / jnp.sqrt(prec_ref[...]), 512)
    jac_ref[...] = jac
    s = plus_diagonal(dot_nt(jac, jac), 1.0 / weight_ref[...].reshape(1, -1)[:, :TOP])
    inv_ref[...] = spd_inverse(tiles_of(s))


def top_step(keep, got, prec, weight):
    return pl.pallas_call(
        top_kernel,
        out_shape=(
            jax.ShapeDtypeStruct((TOP, 512), f32),
            jax.ShapeDtypeStruct((TOP, TOP), f32),
        ),
        cost_estimate=pl.CostEstimate(flops=10**9, bytes_accessed=0, transcendentals=0),
        compiler_params=GRANT,
        name="top_step",
    )(keep, got, prec, weight)


def low_kernel(
    keep_ref, got_ref, top_ref, inv_ref, state_ref, prec_ref, mean_ref, weight_ref,
    out_ref, short_ref,
):
    block = keep_ref[...] + got_ref[...].astype(f32)
    root = jnp.sqrt(prec_ref[...])
    scale = wide(1.0 / root, 512)
    noise = wide(1.0 / weight_ref[...].reshape(1, -1)[:, TOP:], LOW, 1.0)
    low = unfolded(block, LOW, 24) * scale
    top, inv0 = top_ref[...], inv_ref[...]
    first = BLOCK - CUT - 8
    v = [block[first + i : first + i + 1] + block[first + 3 + i : first + 4 + i] for i in range(3)]
    v0 = jnp.broadcast_to(v[0], (8, 128))
    v12 = jnp.broadcast_to(jnp.concatenate(v[1:], axis=1)[:, :LOW], (8, LOW))
    shift = wide(root, 512) * (state_ref[...] - wide(mean_ref[...], 512))
    shift = jnp.broadcast_to(shift, (8, 512))
    both = jnp.concatenate([low, shift], axis=0)
    by_top, by_low = dot_nt(both, top), dot_nt(both, low)
    v0 -= by_top[LOW:]
    v12 -= by_low[LOW:]
    s10 = by_top[:LOW]
    t10 = dot_nn(s10, inv0)
    s = plus_diagonal(by_low[:LOW], noise) - dot_nt(t10, s10)
    v12 -= dot_nt(v0, t10)
    inv1 = spd_inverse(tiles_of(s[:128, :128]))
    s21 = s[128:, :128]
    t21 = dot_nn(s21, inv1)
    s22 = s[128:, 128:] - dot_nt(t21, s21)
    s22 = jnp.pad(s22, ((0, 0), (0, 256 - LOW)))
    v1 = v12[:, :128]
    v2 = v12[:, 128:] - dot_nt(v1, t21)
    inv2 = spd_inverse(tiles_of(s22))[: LOW - 128]
    y2 = dot_nn(v2, inv2)[:, : LOW - 128]
    y1 = dot_nn(v1 - dot_nn(y2, s21), inv1)
    y12 = jnp.concatenate([y1, y2], axis=1)
    y0 = dot_nn(v0 - dot_nn(y12, s10), inv0)
    step = (dot_nn(y0, top) + dot_nn(y12, low)) * scale
    new = wide(mean_ref[...], 512) - step[0:1]
    out_ref[...] = new
    short_ref[...] = new[:, : mean_ref.shape[1]].astype(bf16)


def low_step(keep, got, top, inv0, state, prec, mean, weight):
    return pl.pallas_call(
        low_kernel,
        out_shape=(
            jax.ShapeDtypeStruct(state.shape, f32),
            jax.ShapeDtypeStruct(mean.shape, bf16),
        ),
        cost_estimate=pl.CostEstimate(flops=10**9, bytes_accessed=0, transcendentals=0),
        compiler_params=GRANT,
        input_output_aliases={4: 0},
        name="low_step",
    )(keep, got, top, inv0, state, prec, mean, weight)


def index_of(z, y, core):
    return z * 8 + y * 2 + core


MEMBERS = [(z, y, core) for z in range(2) for y in range(4) for core in range(2)]


def swap_core(value):
    return lax.ppermute(
        value, "chan", [(index_of(z, y, c), index_of(z, y, 1 - c)) for z, y, c in MEMBERS]
    )


def move_y(value, step):
    return lax.ppermute(
        value, "chan", [(index_of(z, y, c), index_of(z, (y + step) % 4, c)) for z, y, c in MEMBERS]
    )


def swap_z(value):
    return lax.ppermute(
        value, "chan", [(index_of(z, y, c), index_of(1 - z, y, c)) for z, y, c in MEMBERS]
    )


def gathered(value):
    pair = jnp.concatenate([value, swap_core(value)], axis=0)
    four = jnp.concatenate([pair, swap_z(pair)], axis=0)
    return [four] + [move_y(four, -dy) for dy in (1, 2, 3)]


def after(value, *others):
    return lax.optimization_barrier((value, *others))[0]


def local(
    observed, eigvec, jacobian, radiance_base, curvature, block_mask,
    pc_weight, prior_prec, prior_mean, state0,
):
    eig_t = eigvec.T
    jac_t = jnp.swapaxes(jacobian, 1, 2)
    prec = prior_prec.reshape(1, -1)

    def iterate(_, carry):
        state, short = carry
        fours = gathered(short)
        valid = valid_channels(after(block_mask, short), observed.shape[1])
        slope, resid = slopes(
            fours, observed, valid, radiance_base, curvature, eig_t, jac_t
        )

        def chip_sum(dy, here):
            keep, send = project(dy, here, resid, eig_t, jac_t)
            return keep, swap_core(send)

        def chunk(pair, part, dz):
            return pair[0][dz, part] + pair[1][dz, part]

        everything = slice(0, BLOCK)
        far = chip_sum(2, slope)
        ahead = chip_sum(1, slope)
        relay = [chunk(far, everything, dz).astype(bf16) for dz in range(2)]
        forth, back = move_y(relay[0], 1), move_y(relay[1], -1)
        later = after(slope, *relay)
        behind = chip_sum(3, later)
        own = chip_sum(0, after(later, behind[0]))
        both, gate = [], later
        for part in (slice(0, CUT), slice(CUT, BLOCK)):
            up = [chunk(ahead, part, 0) + forth[part].astype(f32), chunk(ahead, part, 1)]
            down = [chunk(behind, part, 0), chunk(behind, part, 1) + back[part].astype(f32)]
            up = after(jnp.stack(up).astype(bf16), gate)
            down = gate = jnp.stack(down).astype(bf16)
            up, down = move_y(up, 1), move_y(down, -1)
            near = [
                chunk(own, part, dz) + up[dz].astype(f32) + down[dz].astype(f32)
                for dz in range(2)
            ]
            both.append((near[0], swap_z(near[1].astype(bf16))))
        top, inv0 = top_step(*both[0], prec, pc_weight)
        return low_step(*both[1], top, inv0, state, prec, prior_mean, pc_weight)

    count = state0.shape[1]
    start = (jnp.pad(state0, ((0, 0), (0, 512 - count))), state0.astype(bf16))
    return lax.fori_loop(0, ITERS, iterate, start)[0][:, :count]


def solution(mesh):
    return jax.shard_map(
        local,
        mesh=mesh,
        in_specs=(
            P("prof", "chan"),
            P("chan", None),
            P("prof", "chan", None),
            P("chan"),
            P("chan"),
            P("prof", "chan"),
            P(),
            P(),
            P(("prof", "chan"), None),
            P(("prof", "chan"), None),
        ),
        out_specs=P(("prof", "chan"), None),
        check_vma=False,
    )
```
